32 devices in a mesh: dp: 8 (over y, x, core), tensor: 4 (over z).
Axes of the slice: x: 2, y: 2, z: 4, core: 2. Of those that a mesh axis runs over, the one named last changes fastest.
Arguments:
- tokens: bfloat16 [6400, 1024], P('dp'), may hold values from -10.5 to 10.5, as said below
- blank_mask: int32 [64], P('dp'), may hold values 0 or 1
- norm_gain: float32 [2, 1024], replicated, may hold values from 0.25 to 1.75
- norm_bias: float32 [2, 1024], replicated, may hold values from -1.8 to 1.8
- w_qkv: bfloat16 [3, 1024, 1024], P(None, None, 'tensor'), may hold values from -0.1875 to 0.1875
- qv_bias: float32 [2, 1024], P(None, 'tensor'), may hold values from -1.8 to 1.8
- rel_bias: float32 [32, 361], P('tensor'), may hold values from -5 to 5
- w_out: bfloat16 [1024, 1024], P('tensor'), may hold values from -0.75 to 0.75
- out_bias: float32 [2, 1024], replicated, may hold values from -1.8 to 1.8
- w_up: bfloat16 [1024, 4096], P(None, 'tensor'), may hold values from -0.1875 to 0.1875
- up_bias: float32 [4096], P('tensor'), may hold values from -1.8 to 1.8
- w_down: bfloat16 [4096, 1024], P('tensor'), may hold values from -0.09375 to 0.09375
- grad_out: bfloat16 [6400, 1024], P('dp'), may hold values from -6 to 6
Outputs:
- output: bfloat16 [6400, 1024], P(('dp', 'tensor'))
- grad_tokens: float32 [6400, 1024], P(('dp', 'tensor'))
- grad_norm_gain: float32 [2, 1024], replicated
- grad_norm_bias: float32 [2, 1024], replicated
- grad_w_qkv: float32 [3, 1024, 1024], P(None, None, 'tensor')
- grad_qv_bias: float32 [2, 1024], P(None, 'tensor')
- grad_rel_bias: float32 [32, 361], P('tensor')
- grad_w_out: float32 [1024, 1024], P('tensor')
- grad_out_bias: float32 [2, 1024], replicated
- grad_w_up: float32 [1024, 4096], P(None, 'tensor')
- grad_up_bias: float32 [4096], P('tensor')
- grad_w_down: float32 [4096, 1024], P('tensor')
- root_means: float32 [3], replicated
The draws below stay inside these ranges and needn't reach their ends.
Inputs may be any that keep to these rules, and one draw needn't show every extreme that they name: `tokens`: values are of order one, with row scales differing between windows. `blank_mask`: 1 marks a blank window.
All inputs are finite; a program needn't handle non-finite values. No bound on the sum of `blank_mask` on one device may be relied on, other than what follows from the above.
Results may differ from the reference program's by a relative error of at most 0.0095.
The reference program's roundings to bfloat16 on the way count: a program that leaves them out, or rounds other values in their place, can miss the bound.
Values may be sent and summed in bfloat16 or wider, within the bound.
A program may use at most 128 MiB of HBM per device.

```python
import jax
import jax.numpy as jnp
from jax import lax

D = 1024
HEADS = 32
HEAD_DIM = 32
FF = 4096
WS = 10
WIN_DEV = 8
WINDOWS = 64
TOKENS = 6400
REL = 361
N_DP = 8


def draw_tokens(key, part):
    first_key = jax.random.fold_in(key, 0)
    window_index = (jnp.arange(TOKENS) // (WS * WS)).astype(jnp.float32)
    window_scale = 0.5 * jnp.power(8.0, window_index / max(WINDOWS - 1, 1))
    values_raw = jax.random.truncated_normal(first_key, -2.5, 2.5, (TOKENS, D), jnp.float32)
    return (values_raw * window_scale[:, None]).astype(jnp.bfloat16)


def touch_ends(entries, rng, least, high):
    index_at = [jax.random.randint(jax.random.fold_in(rng, axis), (), 0, length) for axis, length in enumerate(entries.shape)]
    longest = entries.shape.index(max(entries.shape))
    next_to = index_at[:longest] + [(index_at[longest] + 1) % entries.shape[longest]] + index_at[longest + 1:]
    return entries.at[tuple(index_at)].set(least).at[tuple(next_to)].set(high)


def levels(rng, shape, shards, least, largest):
    gain, own = 1.0, jax.random.fold_in(rng, 6)
    for axis_at, blocks in shards:
        heights = jnp.exp(jax.random.uniform(jax.random.fold_in(own, axis_at), (blocks,), jnp.float32, least / len(shards), largest / len(shards)))
        gain = gain * jnp.repeat(heights, shape[axis_at] // blocks).reshape([-1 if axis == axis_at else 1 for axis in range(len(shape))])
    return gain


def normal_values(rng, extent, deviation, most, pieces=(), kind=jnp.bfloat16):
    level = levels(rng, extent, pieces, -0.22, 0.18) if pieces else 1.0
    array = jax.random.normal(rng, extent, jnp.float32) * deviation * level
    return jnp.minimum(jnp.maximum(array, -most), most).astype(kind)


def setup_inputs(seed: int = 0) -> dict:
    key_list = jax.random.split(jax.random.key(seed), 14)
    tokens = draw_tokens(jax.random.fold_in(key_list[13], 71), 0)
    blank_mask = touch_ends((jax.random.randint(key_list[1], (WINDOWS,), 0, 2) < 1).astype(jnp.int32), jax.random.fold_in(key_list[1], 1), 0, 1)
    norm_gain = jnp.clip(1.0 + 0.15 * jax.random.normal(key_list[2], (2, D), jnp.float32), 0.25, 1.75)
    norm_bias = normal_values(key_list[3], (2, D), 0.3, 1.8, (), jnp.float32)
    w_qkv = normal_values(key_list[4], (3, D, D), D ** -0.5, 0.1875, ((2, 4),))
    qv_bias = normal_values(key_list[5], (2, D), 0.3, 1.8, ((1, 4),), jnp.float32)
    rel_bias = normal_values(key_list[6], (HEADS, REL), 1.0, 5.0, ((0, 4),), jnp.float32)
    w_out = normal_values(key_list[7], (D, D), (D // 16) ** -0.5, 0.75, ((0, 4),))
    out_bias = normal_values(key_list[8], (2, D), 0.3, 1.8, (), jnp.float32)
    w_up = normal_values(key_list[9], (D, FF), D ** -0.5, 0.1875, ((1, 4),))
    up_bias = normal_values(key_list[10], (FF,), 0.3, 1.8, ((0, 4),), jnp.float32)
    w_down = normal_values(key_list[11], (FF, D), FF ** -0.5, 0.09375, ((0, 4),))
    grad_out = normal_values(key_list[12], (TOKENS, D), 1.0, 6.0, ((0, 8),))
    return dict(tokens=tokens, blank_mask=blank_mask, norm_gain=norm_gain, norm_bias=norm_bias, w_qkv=w_qkv, qv_bias=qv_bias, rel_bias=rel_bias, w_out=w_out, out_bias=out_bias, w_up=w_up, up_bias=up_bias, w_down=w_down, grad_out=grad_out)


highest = lax.Precision.HIGHEST
norm_eps = 1e-05

@jax.custom_vjp
def low(v):
    return lax.optimization_barrier(v.astype(jnp.bfloat16)).astype(jnp.float32)

@jax.custom_vjp
def low_back(v):
    return v

def low_keep(v):
    return (low(v), None)

def low_pass(kept, grad):
    return (grad,)

def back_keep(v):
    return (v, None)

def back_low(kept, grad):
    return (low(grad),)
low.defvjp(low_keep, low_pass)
low_back.defvjp(back_keep, back_low)

def layer_norm(values, gain_row, shift_row):
    center = lax.optimization_barrier(jnp.mean(values, axis=-1, keepdims=True))
    shifted = values - center
    spread = lax.optimization_barrier(jnp.mean(shifted * shifted, axis=-1, keepdims=True))
    return shifted * lax.rsqrt(spread + norm_eps) * gain_row + shift_row

def relative_onehot(window_side):
    positions = jnp.arange(window_side)
    offset_grid = positions[:, None] - positions[None, :] + (window_side - 1)
    return (offset_grid[:, :, None] == jnp.arange(2 * window_side - 1)[None, None, :]).astype(jnp.float32)

def relative(bias_table, window_side):
    onehot = relative_onehot(window_side)
    heads_count = bias_table.shape[0]
    square = bias_table.reshape(heads_count, 2 * window_side - 1, 2 * window_side - 1)
    spread_full = jnp.einsum('ija,klb,hab->hikjl', onehot, onehot, square, precision=highest)
    return spread_full.reshape(heads_count, window_side * window_side, window_side * window_side)

def forward(source, norm_gain, norm_bias, w_qkv, qv_bias, rel_bias, w_out, out_bias, w_up, up_bias, w_down):
    normed_one = low(layer_norm(source, norm_gain[0], norm_bias[0]))
    projected = jnp.einsum('rd,tde->tre', normed_one, w_qkv, precision=highest)
    shifts = jnp.stack([qv_bias[0], jnp.zeros_like(qv_bias[0]), qv_bias[1]])
    projected = low_back(low(projected + shifts[:, None, :]))
    grouped = projected.reshape(3, N_DP, WIN_DEV, WS * WS, HEADS, HEAD_DIM)
    grouped = jnp.moveaxis(grouped, 1, 0)
    bias_block = relative(rel_bias, WS)
    score_scale = HEAD_DIM ** (-0.5)

    def attend(window_block):
        scores = jnp.einsum('wihc,wjhc->whij', window_block[0], window_block[1], precision=highest) * score_scale + bias_block[None]
        scores = low_back(scores)
        weights = low(jax.nn.softmax(scores, axis=-1))
        mixed_heads = jnp.einsum('whij,wjhc->wihc', weights, window_block[2], precision=highest)
        return low_back(low(mixed_heads))
    mixed_heads = lax.map(jax.checkpoint(attend), grouped).reshape(TOKENS, D)
    attn_branch = low_back(jnp.dot(mixed_heads, w_out, precision=highest) + out_bias[0])
    resid_one = source + attn_branch
    normed_two = low(layer_norm(resid_one, norm_gain[1], norm_bias[1]))
    hidden = low_back(jnp.dot(normed_two, w_up, precision=highest) + up_bias)
    active = low(jax.nn.gelu(hidden, approximate=False))
    mlp_branch = low_back(jnp.dot(active, w_down, precision=highest) + out_bias[1])
    return (resid_one + mlp_branch, (attn_branch, mlp_branch))

def reference(tokens, blank_mask, norm_gain, norm_bias, w_qkv, qv_bias, rel_bias, w_out, out_bias, w_up, up_bias, w_down, grad_out):
    floats = [array_item.astype(jnp.float32) for array_item in (tokens, norm_gain, norm_bias, w_qkv, qv_bias, rel_bias, w_out, out_bias, w_up, up_bias, w_down)]
    output, pull_back, extras = jax.vjp(forward, *floats, has_aux=True)
    gradients = pull_back(grad_out.astype(jnp.float32))
    alive_rows = jnp.repeat(1.0 - blank_mask.astype(jnp.float32), WS * WS)[:, None]
    live_count = jnp.maximum(jnp.sum(alive_rows), 1.0) * D

    def root_mean(values):
        return jnp.sqrt(jnp.sum(alive_rows * values * values) / live_count)
    root_means = jnp.stack([root_mean(floats[0]), root_mean(extras[0]), root_mean(extras[1])])
    return (output.astype(jnp.bfloat16), gradients[0], gradients[1], gradients[2], gradients[3], gradients[4], gradients[5], gradients[6], gradients[7], gradients[8], gradients[9], gradients[10], root_means)
```

```python
import jax
import jax.numpy as jnp
from jax import lax
from jax.sharding import PartitionSpec as P

WS = 10


highest = lax.Precision.HIGHEST
norm_eps = 1e-05
half_root = 0.7071067811865476
gauss_norm = 0.3989422804014327


def normalize(values):
    center = jnp.mean(values, axis=-1, keepdims=True)
    shifted = values - center
    spread = jnp.mean(shifted * shifted, axis=-1, keepdims=True)
    inverse = lax.rsqrt(spread + norm_eps)
    return (shifted * inverse, inverse)


def norm_back(gradient, normed_hat, inverse, gain_row):
    scaled = gradient * gain_row
    inner_sum = jnp.mean(scaled, axis=-1, keepdims=True)
    cross_sum = jnp.mean(scaled * normed_hat, axis=-1, keepdims=True)
    return inverse * (scaled - inner_sum - normed_hat * cross_sum)


def relative_onehot(window_side):
    positions = jnp.arange(window_side)
    offset_grid = positions[:, None] - positions[None, :] + (window_side - 1)
    return (offset_grid[:, :, None] == jnp.arange(2 * window_side - 1)[None, None, :]).astype(
        jnp.float32
    )


def relative(bias_table, window_side):
    onehot = relative_onehot(window_side)
    heads_count = bias_table.shape[0]
    square = bias_table.reshape(heads_count, 2 * window_side - 1, 2 * window_side - 1)
    spread_full = jnp.einsum("ija,klb,hab->hikjl", onehot, onehot, square, precision=highest)
    return spread_full.reshape(heads_count, window_side * window_side, window_side * window_side)


def relative_back(gradient, window_side):
    onehot = relative_onehot(window_side)
    heads_count = gradient.shape[0]
    grad_grid = gradient.reshape(heads_count, window_side, window_side, window_side, window_side)
    folded = jnp.einsum("hikjl,ija,klb->hab", grad_grid, onehot, onehot, precision=highest)
    return folded.reshape(heads_count, (2 * window_side - 1) ** 2)


def scatter_rows(part):
    sums = lax.psum_scatter(
        part.astype(jnp.bfloat16), "tensor", scatter_dimension=0, tiled=True
    )
    return sums.astype(jnp.float32)


def on_device(
    tokens,
    blank_mask,
    norm_gain,
    norm_bias,
    w_qkv,
    qv_bias,
    rel_bias,
    w_out,
    out_bias,
    w_up,
    up_bias,
    w_down,
    grad_out,
):
    tensor_count = lax.axis_size("tensor")
    rows_all = tokens.shape[0]
    rows_own = rows_all // tensor_count
    row_start = lax.axis_index("tensor") * rows_own
    window_area = WS * WS
    windows = rows_all // window_area
    heads_here = rel_bias.shape[0]
    width_here = w_out.shape[0]
    head_dim = width_here // heads_here
    score_scale = head_dim ** (-0.5)

    def own_rows(values):
        return lax.dynamic_slice_in_dim(values, row_start, rows_own, 0)

    source = tokens.astype(jnp.float32)
    hat_one, inv_one = normalize(source)
    normed_one = (hat_one * norm_gain[0] + norm_bias[0]).astype(jnp.bfloat16)
    projected = jnp.einsum("rd,tde->tre", normed_one, w_qkv, preferred_element_type=jnp.float32)
    shifts = jnp.stack([qv_bias[0], jnp.zeros_like(qv_bias[0]), qv_bias[1]])
    projected = (projected + shifts[:, None, :]).astype(jnp.bfloat16)
    projected = projected.reshape(3, windows, window_area, heads_here, head_dim)
    query_part, key_part, value_part = (projected[0], projected[1], projected[2])
    bias_block = relative(rel_bias, WS)

    def scores_of():
        raw_scores = jnp.einsum(
            "wihc,wjhc->whij", query_part, key_part, preferred_element_type=jnp.float32
        )
        return raw_scores * score_scale + bias_block[None]

    scores = scores_of()
    row_top = jnp.max(scores, axis=-1, keepdims=True)
    exponent = jnp.exp(scores - row_top)
    row_total = jnp.sum(exponent, axis=-1, keepdims=True)
    log_total = row_top + jnp.log(row_total)
    weights = (exponent / row_total).astype(jnp.bfloat16)
    mixed_heads = jnp.einsum(
        "whij,wjhc->wihc", weights, value_part, preferred_element_type=jnp.float32
    )
    mixed_heads = mixed_heads.astype(jnp.bfloat16).reshape(rows_all, width_here)
    attn_part = jnp.dot(mixed_heads, w_out, preferred_element_type=jnp.float32)
    alive_rows = jnp.repeat(1.0 - blank_mask.astype(jnp.float32), window_area)
    alive_own = own_rows(alive_rows)[:, None]
    source_own = own_rows(source)
    attn_own = scatter_rows(attn_part) + out_bias[0]
    resid_own = source_own + attn_own
    hat_two, inv_two = normalize(resid_own)
    normed_rows = (hat_two * norm_gain[1] + norm_bias[1]).astype(jnp.bfloat16)
    normed_two = lax.all_gather(normed_rows, "tensor", axis=0, tiled=True)
    hidden = jnp.dot(normed_two, w_up, preferred_element_type=jnp.float32) + up_bias
    active = jax.nn.gelu(hidden, approximate=False).astype(jnp.bfloat16)
    mlp_part = jnp.dot(active, w_down, preferred_element_type=jnp.float32)
    branch_own = scatter_rows(mlp_part) + out_bias[1]
    output = (resid_own + branch_own).astype(jnp.bfloat16)
    stat_terms = jnp.stack(
        [
            jnp.sum(alive_own * source_own * source_own),
            jnp.sum(alive_own * attn_own * attn_own),
            jnp.sum(alive_own * branch_own * branch_own),
            jnp.sum(alive_own),
        ]
    )
    stat_total = lax.psum(stat_terms, ("dp", "tensor"))
    grad_full = grad_out.astype(jnp.float32)
    grad_down = jnp.einsum("rf,rd->fd", active, grad_out, preferred_element_type=jnp.float32)
    grad_active = jnp.einsum("rd,fd->rf", grad_out, w_down, preferred_element_type=jnp.float32)
    gelu_slope = (
        0.5 * (1.0 + lax.erf(hidden * half_root))
        + hidden * jnp.exp(-0.5 * hidden * hidden) * gauss_norm
    )
    grad_hidden = (grad_active * gelu_slope).astype(jnp.bfloat16)
    grad_up_bias = jnp.sum(grad_hidden.astype(jnp.float32), axis=0)
    grad_up = jnp.einsum("rd,rf->df", normed_two, grad_hidden, preferred_element_type=jnp.float32)
    norm_part = jnp.einsum("rf,df->rd", grad_hidden, w_up, preferred_element_type=jnp.float32)
    grad_norm_own = scatter_rows(norm_part)
    grad_resid_own = own_rows(grad_full) + norm_back(grad_norm_own, hat_two, inv_two, norm_gain[1])
    grad_attn = lax.all_gather(grad_resid_own.astype(jnp.bfloat16), "tensor", axis=0, tiled=True)
    gain_two = jnp.sum(grad_norm_own * hat_two, axis=0)
    shift_two = jnp.sum(grad_norm_own, axis=0)
    attn_bias_term = jnp.sum(own_rows(grad_attn).astype(jnp.float32), axis=0)
    mlp_bias_term = jnp.sum(own_rows(grad_full), axis=0)
    grad_wout = jnp.einsum("re,rd->ed", mixed_heads, grad_attn, preferred_element_type=jnp.float32)
    grad_mixed = jnp.einsum("rd,ed->re", grad_attn, w_out, preferred_element_type=jnp.float32)
    grad_mixed = grad_mixed.astype(jnp.bfloat16).reshape(windows, window_area, heads_here, head_dim)
    probs_full = jnp.exp(scores_of() - log_total)
    probs_low = probs_full.astype(jnp.bfloat16)
    grad_values = jnp.einsum(
        "whij,wihc->wjhc", probs_low, grad_mixed, preferred_element_type=jnp.float32
    )
    grad_probs = jnp.einsum(
        "wihc,wjhc->whij", grad_mixed, value_part, preferred_element_type=jnp.float32
    )
    inner_sum = jnp.sum(grad_probs * probs_full, axis=-1, keepdims=True)
    grad_scores = (probs_full * (grad_probs - inner_sum)).astype(jnp.bfloat16)
    grad_table = relative_back(jnp.sum(grad_scores.astype(jnp.float32), axis=0), WS)
    grad_query = (
        jnp.einsum("whij,wjhc->wihc", grad_scores, key_part, preferred_element_type=jnp.float32)
        * score_scale
    )
    grad_keys = (
        jnp.einsum("whij,wihc->wjhc", grad_scores, query_part, preferred_element_type=jnp.float32)
        * score_scale
    )
    grad_proj = (
        jnp.stack([grad_query, grad_keys, grad_values])
        .astype(jnp.bfloat16)
        .reshape(3, rows_all, width_here)
    )
    grad_qv = jnp.stack(
        [
            jnp.sum(grad_proj[0].astype(jnp.float32), axis=0),
            jnp.sum(grad_proj[2].astype(jnp.float32), axis=0),
        ]
    )
    grad_qkv = jnp.einsum("rd,tre->tde", normed_one, grad_proj, preferred_element_type=jnp.float32)
    input_part = jnp.einsum("tre,tde->rd", grad_proj, w_qkv, preferred_element_type=jnp.float32)
    grad_in_own = scatter_rows(input_part)
    hat_one_own = own_rows(hat_one)
    grad_tokens = grad_resid_own + norm_back(
        grad_in_own, hat_one_own, own_rows(inv_one), norm_gain[0]
    )
    gain_one = jnp.sum(grad_in_own * hat_one_own, axis=0)
    shift_one = jnp.sum(grad_in_own, axis=0)
    gain_terms = jnp.stack([gain_one, gain_two])
    shift_terms = jnp.stack([shift_one, shift_two])
    bias_terms = jnp.stack([attn_bias_term, mlp_bias_term])
    gain_sums, shift_sums, bias_sums = lax.psum(
        (gain_terms, shift_terms, bias_terms), ("dp", "tensor")
    )
    grad_qv, grad_table, grad_up_bias = lax.psum((grad_qv, grad_table, grad_up_bias), "dp")
    grad_qkv, grad_wout, grad_up, grad_down = [
        total.astype(jnp.float32)
        for total in lax.psum(
            [part.astype(jnp.bfloat16) for part in (grad_qkv, grad_wout, grad_up, grad_down)],
            "dp",
        )
    ]
    live_count = jnp.maximum(stat_total[3], 1.0) * tokens.shape[1]
    root_means = jnp.sqrt(stat_total[0:3] / live_count)
    return (
        output,
        grad_tokens,
        gain_sums,
        shift_sums,
        grad_qkv,
        grad_qv,
        grad_table,
        grad_wout,
        bias_sums,
        grad_up,
        grad_up_bias,
        grad_down,
        root_means,
    )


def solution(mesh):
    in_specs = (
        P("dp", None),
        P("dp"),
        P(),
        P(),
        P(None, None, "tensor"),
        P(None, "tensor"),
        P("tensor", None),
        P("tensor", None),
        P(),
        P(None, "tensor"),
        P("tensor"),
        P("tensor", None),
        P("dp", None),
    )
    out_specs = (
        P(("dp", "tensor"), None),
        P(("dp", "tensor"), None),
        P(),
        P(),
        P(None, None, "tensor"),
        P(None, "tensor"),
        P("tensor", None),
        P("tensor", None),
        P(),
        P(None, "tensor"),
        P("tensor"),
        P("tensor", None),
        P(),
    )
    return jax.shard_map(
        on_device, mesh=mesh, in_specs=in_specs, out_specs=out_specs, check_vma=False
    )
```

```python
import functools

import jax
import jax.numpy as jnp
from jax import lax
from jax.experimental import pallas as pl
from jax.experimental.pallas import tpu as pltpu
from jax.sharding import PartitionSpec as P


WS = 10


MESH_ID = pl.DeviceIdType.MESH
half_root = 0.7071067811865476
gauss_norm = 0.3989422804014327
norm_eps = 1e-05
ROW_TILE = 16
BLOCKS = 8


def last_dims(left, right):
    return lax.dot_general(
        left, right, (((1,), (1,)), ((), ())), preferred_element_type=jnp.float32
    )


def first_dims(left, right):
    return lax.dot_general(
        left, right, (((0,), (0,)), ((), ())), preferred_element_type=jnp.float32
    )


def remote(src, dst, sent, got, target):
    return pltpu.make_async_remote_copy(
        src_ref=src,
        dst_ref=dst,
        send_sem=sent,
        recv_sem=got,
        device_id=target,
        device_id_type=MESH_ID,
    )


def cube_place():
    place = lax.axis_index("dp")
    core = lax.rem(place, 2)
    along_x = lax.rem(place // 2, 2)
    along_y = place // 4
    peers = (
        {"dp": place + 1 - 2 * core},
        {"dp": place + 2 - 4 * along_x},
        {"dp": place + 4 - 8 * along_y},
    )
    return (core, along_x, along_y), peers


def entry_barrier(count, peers, everyone):
    here = lax.axis_index("tensor")
    barrier = pltpu.get_barrier_semaphore()
    for peer in peers:
        pl.semaphore_signal(barrier, inc=1, device_id=peer, device_id_type=MESH_ID)
    if everyone:
        for step in range(1, count):
            other = {"tensor": lax.rem(here + step, count)}
            pl.semaphore_signal(barrier, inc=1, device_id=other, device_id_type=MESH_ID)
        pl.semaphore_wait(barrier, len(peers) + count - 1)
        return
    for ahead in (-1, 1):
        other = here + ahead

        @pl.when((other >= 0) & (other < count))
        def _():
            pl.semaphore_signal(
                barrier, inc=1, device_id={"tensor": other}, device_id_type=MESH_ID
            )

    ends = jnp.where(here > 0, 1, 0) + jnp.where(here < count - 1, 1, 0)
    pl.semaphore_wait(barrier, len(peers) + ends)


class LineSum:
    def __init__(self, count, subs, rows, part, up, down, sems):
        self.count, self.subs, self.rows = count, subs, rows
        self.part, self.up, self.down = part, up, down
        self.up_sent, self.up_got, self.down_sent, self.down_got = sems
        self.here = lax.axis_index("tensor")

    def copy(self, src, owner, sub, ahead):
        spot = pl.ds(sub * self.rows, self.rows)
        landing = self.up if ahead > 0 else self.down
        sent = self.up_sent if ahead > 0 else self.down_sent
        got = self.up_got if ahead > 0 else self.down_got
        return remote(
            src.at[owner, spot],
            landing.at[owner, spot],
            sent.at[owner, sub],
            got.at[owner, sub],
            {"tensor": self.here + ahead},
        )

    def send(self, owner, sub, ahead):
        outer = 0 if ahead > 0 else self.count - 1
        inside = (self.here < owner) if ahead > 0 else (self.here > owner)
        landing = self.up if ahead > 0 else self.down
        spot = pl.ds(sub * self.rows, self.rows)

        @pl.when(inside & (self.here == outer))
        def _():
            self.copy(self.part, owner, sub, ahead).start()

        @pl.when(inside & (self.here != outer))
        def _():
            self.copy(self.part, owner, sub, ahead).wait_recv()
            total = landing[owner, spot].astype(jnp.float32) + self.part[owner, spot].astype(
                jnp.float32
            )
            landing[owner, spot] = total.astype(jnp.bfloat16)
            self.copy(landing, owner, sub, ahead).start()

    def step(self, turn):
        for sub in range(self.subs):
            self.send(self.count - turn, sub, 1)
            self.send(turn - 1, sub, -1)

    def collect(self, sub, total_ref):
        spot = pl.ds(sub * self.rows, self.rows)
        here = self.here

        @pl.when(here > 0)
        def _():
            self.copy(self.part, here, sub, 1).wait_recv()
            total_ref[spot] += self.up[here, spot].astype(jnp.float32)

        @pl.when(here < self.count - 1)
        def _():
            self.copy(self.part, here, sub, -1).wait_recv()
            total_ref[spot] += self.down[here, spot].astype(jnp.float32)

    def drain(self):
        for owner in range(self.count):
            for sub in range(self.subs):

                @pl.when(self.here < owner)
                def _():
                    self.copy(self.part, owner, sub, 1).wait_send()

                @pl.when(self.here > owner)
                def _():
                    self.copy(self.part, owner, sub, -1).wait_send()


class LineGather:
    def __init__(self, count, subs, rows, whole, sems):
        self.count, self.subs, self.rows, self.whole = count, subs, rows, whole
        self.up_sent, self.up_got, self.down_sent, self.down_got = sems
        self.here = lax.axis_index("tensor")

    def copy(self, owner, sub, ahead):
        spot = pl.ds(sub * self.rows, self.rows)
        sent = self.up_sent if ahead > 0 else self.down_sent
        got = self.up_got if ahead > 0 else self.down_got
        return remote(
            self.whole.at[owner, spot],
            self.whole.at[owner, spot],
            sent.at[owner, sub],
            got.at[owner, sub],
            {"tensor": self.here + ahead},
        )

    def send_own(self, sub):
        @pl.when(self.here < self.count - 1)
        def _():
            self.copy(self.here, sub, 1).start()

        @pl.when(self.here > 0)
        def _():
            self.copy(self.here, sub, -1).start()

    def step(self, far):
        here, count = self.here, self.count
        for sub in range(self.subs):

            @pl.when(here - far >= 0)
            def _():
                self.copy(here - far, sub, 1).wait_recv()

                @pl.when(here < count - 1)
                def _():
                    self.copy(here - far, sub, 1).start()

            @pl.when(here + far < count)
            def _():
                self.copy(here + far, sub, -1).wait_recv()

                @pl.when(here > 0)
                def _():
                    self.copy(here + far, sub, -1).start()

    def drain(self):
        here, count = self.here, self.count
        for far in range(count):
            for sub in range(self.subs):

                @pl.when((here - far >= 0) & (here < count - 1))
                def _():
                    self.copy(here - far, sub, 1).wait_send()

                @pl.when((here + far < count) & (here > 0))
                def _():
                    self.copy(here + far, sub, -1).wait_send()


class CubeSum:
    def __init__(self, order, part, landings, total, sems):
        bits, peers = cube_place()
        self.bits = [bits[axis] for axis in order]
        self.peers = [peers[axis] for axis in order]
        self.part, self.landings, self.total = part, landings, total
        self.out_sent, self.out_got, self.back_sent, self.back_got = sems

    def span(self, level, mine):
        start = 0
        for at in range(level + 1):
            bit = self.bits[at]
            if at == level and not mine:
                bit = 1 - bit
            start = start + bit * (BLOCKS >> (at + 1))
        return start

    def out(self, level):
        size = BLOCKS >> (level + 1)
        return remote(
            self.part.at[pl.ds(self.span(level, False), size)],
            self.landings[level],
            self.out_sent.at[level],
            self.out_got.at[level],
            self.peers[level],
        )

    def back(self, level):
        size = BLOCKS >> (level + 1)
        spot = pl.ds(self.span(level, True), size)
        return remote(
            self.total.at[spot],
            self.total.at[spot],
            self.back_sent.at[level],
            self.back_got.at[level],
            self.peers[level],
        )

    def start(self):
        self.out(0).start()

    def reduce(self, level):
        self.out(level).wait_recv()
        size = BLOCKS >> (level + 1)
        base = self.span(level, True)
        into = self.total if level == 2 else self.part

        @pl.loop(0, size)
        def _(at):
            into[base + at] = (
                self.part[base + at].astype(jnp.float32)
                + self.landings[level][at].astype(jnp.float32)
            ).astype(jnp.bfloat16)

        if level < 2:
            self.out(level + 1).start()
        else:
            self.back(2).start()

    def spread(self, level):
        self.back(level).wait_recv()
        if level > 0:
            self.back(level - 1).start()

    def drain(self):
        for level in range(3):
            self.out(level).wait_send()
            self.back(level).wait_send()


def normal_rows(values):
    center = jnp.mean(values, axis=-1, keepdims=True)
    shifted = values - center
    spread = jnp.mean(shifted * shifted, axis=-1, keepdims=True)
    inverse = lax.rsqrt(spread + norm_eps)
    return shifted * inverse, inverse


def back_rows(gradient, hat, inverse, gain_row):
    scaled = gradient * gain_row
    inner = jnp.mean(scaled, axis=-1, keepdims=True)
    cross = jnp.mean(scaled * hat, axis=-1, keepdims=True)
    return inverse * (scaled - inner - hat * cross)


def middle_kernel(
    count,
    subs,
    rows,
    part_ref,
    source_ref,
    live_ref,
    gain_ref,
    shift_ref,
    bias_ref,
    up_ref,
    up_bias_ref,
    down_ref,
    cot_ref,
    output_ref,
    resid_back_ref,
    cot_attn_ref,
    grads_ref,
    sums_ref,
    normed_ref,
    active_ref,
    norm_part_ref,
    mlp_part_ref,
    attn_up,
    attn_down,
    norm_up,
    norm_down,
    mlp_up,
    mlp_down,
    hidden_back_ref,
    total_ref,
    resid_ref,
    hat_ref,
    inverse_ref,
    down_grad_ref,
    up_grad_ref,
    down_land0,
    down_land1,
    down_land2,
    up_land0,
    up_land1,
    up_land2,
    line_sems,
    cube_sems,
):
    here = lax.axis_index("tensor")
    width = up_ref.shape[1]
    tile = 256

    def sems(which):
        return [line_sems.at[4 * which + at] for at in range(4)]

    def cubes(which):
        return [cube_sems.at[4 * which + at] for at in range(4)]

    attn_sum = LineSum(count, subs, rows, part_ref, attn_up, attn_down, sems(0))
    gather = LineGather(count, subs, rows, normed_ref, sems(1))
    norm_sum = LineSum(count, subs, rows, norm_part_ref, norm_up, norm_down, sems(2))
    mlp_sum = LineSum(count, subs, rows, mlp_part_ref, mlp_up, mlp_down, sems(3))
    back_gather = LineGather(count, subs, rows, cot_attn_ref, sems(4))
    down_cube = CubeSum(
        (0, 1, 2),
        down_grad_ref,
        (down_land0, down_land1, down_land2),
        grads_ref.at[0],
        cubes(0),
    )
    up_cube = CubeSum(
        (0, 2, 1), up_grad_ref, (up_land0, up_land1, up_land2), grads_ref.at[1], cubes(1)
    )
    entry_barrier(count, cube_place()[1], False)

    for turn in range(1, count):
        attn_sum.step(turn)
    total_ref[...] = part_ref[here].astype(jnp.float32)
    sums_ref[...] = jnp.zeros_like(sums_ref)
    gain_row, shift_row = gain_ref[1:2, :], shift_ref[1:2, :]
    for sub in range(subs):
        spot = pl.ds(sub * rows, rows)
        attn_sum.collect(sub, total_ref)
        attn = total_ref[spot] + bias_ref[0:1, :]
        source = source_ref[spot].astype(jnp.float32)
        live = live_ref[spot]
        resid = source + attn
        hat, inverse = normal_rows(resid)
        normed_ref[here, spot] = (hat * gain_row + shift_row).astype(jnp.bfloat16)
        gather.send_own(sub)
        resid_ref[spot] = resid
        hat_ref[spot] = hat
        inverse_ref[spot] = inverse
        sums_ref[5:6, :] += jnp.sum(live * source * source, axis=0, keepdims=True)
        sums_ref[6:7, :] += jnp.sum(live * attn * attn, axis=0, keepdims=True)

    def feed(owner):
        @pl.loop(0, width // tile)
        def _(block):
            cols = pl.ds(pl.multiple_of(block * tile, tile), tile)
            hidden = (
                jnp.dot(normed_ref[owner], up_ref[:, cols], preferred_element_type=jnp.float32)
                + up_bias_ref[:, cols]
            )
            cumulative = 0.5 * (1.0 + lax.erf(hidden * half_root))
            active_ref[owner, :, cols] = (hidden * cumulative).astype(jnp.bfloat16)
            slope = cumulative + hidden * jnp.exp(-0.5 * hidden * hidden) * gauss_norm
            grad_active = last_dims(cot_ref[owner], down_ref[cols, :])
            hidden_back_ref[owner, :, cols] = (grad_active * slope).astype(jnp.bfloat16)

        @pl.loop(0, down_ref.shape[1] // tile)
        def _(block):
            cols = pl.ds(pl.multiple_of(block * tile, tile), tile)
            norm_part_ref[owner, :, cols] = last_dims(
                hidden_back_ref[owner], up_ref[cols, :]
            ).astype(jnp.bfloat16)

    def feed_out(owner):
        @pl.loop(0, down_ref.shape[1] // tile)
        def _(block):
            cols = pl.ds(pl.multiple_of(block * tile, tile), tile)
            mlp_part_ref[owner, :, cols] = jnp.dot(
                active_ref[owner], down_ref[:, cols], preferred_element_type=jnp.float32
            ).astype(jnp.bfloat16)

    feed(here)

    @pl.loop(1, count)
    def _(far):
        gather.step(far)

        @pl.loop(0, 2)
        def _(side):
            owner = here + far * (2 * side - 1)

            @pl.when((owner >= 0) & (owner < count))
            def _():
                feed(owner)

    norm_sum.step(1)

    def weight_grad(which, block):
        cols = pl.ds(pl.multiple_of(block * tile, tile), tile)
        flat = (count * subs * rows, width)
        if which:
            left, right = normed_ref, hidden_back_ref
        else:
            left, right = active_ref, cot_ref
        value = first_dims(left[:, :, cols].reshape(flat[0], tile), right[...].reshape(flat))
        into = up_grad_ref if which else down_grad_ref
        value = value.astype(jnp.bfloat16)
        into[2 * block] = value[: tile // 2]
        into[2 * block + 1] = value[tile // 2 :]

    for turn in range(2, count):
        @pl.loop(2 * turn - 4, 2 * turn - 2)
        def _(block):
            weight_grad(0, block)

        norm_sum.step(turn)
    down_cube.start()
    pl.loop(0, count)(feed_out)
    total_ref[...] = norm_part_ref[here].astype(jnp.float32)
    sums_ref[4:5, :] = jnp.sum(
        jnp.sum(hidden_back_ref[...].astype(jnp.float32), axis=0), axis=0, keepdims=True
    )
    for sub in range(subs):
        spot = pl.ds(sub * rows, rows)
        norm_sum.collect(sub, total_ref)
        grad_norm = total_ref[spot]
        hat = hat_ref[spot]
        cot = cot_ref[here, spot].astype(jnp.float32)
        resid_back = cot + back_rows(grad_norm, hat, inverse_ref[spot], gain_row)
        low = resid_back.astype(jnp.bfloat16)
        cot_attn_ref[here, spot] = low
        back_gather.send_own(sub)
        resid_back_ref[spot] = resid_back
        sums_ref[0:1, :] += jnp.sum(grad_norm * hat, axis=0, keepdims=True)
        sums_ref[1:2, :] += jnp.sum(grad_norm, axis=0, keepdims=True)
        sums_ref[2:3, :] += jnp.sum(low.astype(jnp.float32), axis=0, keepdims=True)
        sums_ref[3:4, :] += jnp.sum(cot, axis=0, keepdims=True)

    mlp_sum.step(1)

    @pl.loop(0, width // tile)
    def _(block):
        weight_grad(1, block)

    up_cube.start()
    down_cube.reduce(0)
    for far in range(1, count):
        back_gather.step(far)
        if far + 1 < count:
            mlp_sum.step(far + 1)
        if far == 1:
            up_cube.reduce(0)
            down_cube.reduce(1)
        if far == 2:
            up_cube.reduce(1)
            down_cube.reduce(2)
            up_cube.reduce(2)
    down_cube.spread(2)
    up_cube.spread(2)
    total_ref[...] = mlp_part_ref[here].astype(jnp.float32)
    for sub in range(subs):
        spot = pl.ds(sub * rows, rows)
        mlp_sum.collect(sub, total_ref)
        branch = total_ref[spot] + bias_ref[1:2, :]
        output_ref[spot] = (resid_ref[spot] + branch).astype(jnp.bfloat16)
        sums_ref[7:8, :] += jnp.sum(live_ref[spot] * branch * branch, axis=0, keepdims=True)
    for level in (1, 0):
        down_cube.spread(level)
        up_cube.spread(level)
    for each in (attn_sum, gather, norm_sum, mlp_sum, back_gather, down_cube, up_cube):
        each.drain()


def middle(count, part, source, live, gain, shift, bias, up, up_bias, down, cot, subs, rows):
    depth, width = up.shape
    own = subs * rows
    half = jnp.bfloat16

    def vmem(*shape, kind=half):
        return pltpu.VMEM(shape, kind)

    whole = (count, own, depth)
    blocks = depth // BLOCKS
    spec = pl.BlockSpec(memory_space=pltpu.VMEM)
    landings = [vmem(BLOCKS >> (level + 1), blocks, depth) for level in range(3)]
    return pl.pallas_call(
        functools.partial(middle_kernel, count, subs, rows),
        name="middle",
        out_shape=(
            jax.ShapeDtypeStruct((own, depth), half),
            jax.ShapeDtypeStruct((own, depth), jnp.float32),
            jax.ShapeDtypeStruct(whole, half),
            jax.ShapeDtypeStruct((2, BLOCKS, blocks, depth), half),
            jax.ShapeDtypeStruct((8, depth), jnp.float32),
        ),
        in_specs=[spec] * 10,
        out_specs=(spec,) * 5,
        scratch_shapes=[vmem(*whole)] * 4
        + [vmem(*whole)] * 6
        + [
            vmem(*whole),
            vmem(own, depth, kind=jnp.float32),
            vmem(own, depth, kind=jnp.float32),
            vmem(own, depth, kind=jnp.float32),
            vmem(own, 1, kind=jnp.float32),
            vmem(BLOCKS, blocks, depth),
            vmem(BLOCKS, blocks, depth),
        ]
        + landings
        + landings
        + [
            pltpu.SemaphoreType.DMA((20, count, subs)),
            pltpu.SemaphoreType.DMA((8, 3)),
        ],
        compiler_params=pltpu.CompilerParams(
            collective_id=0, has_side_effects=True, vmem_limit_bytes=67043328
        ),
    )(part, source, live, gain, shift, bias, up, up_bias, down, cot)


highest = lax.Precision.HIGHEST


def normalize(values):
    center = jnp.mean(values, axis=-1, keepdims=True)
    shifted = values - center
    spread = jnp.mean(shifted * shifted, axis=-1, keepdims=True)
    inverse = lax.rsqrt(spread + norm_eps)
    return (shifted * inverse, inverse)


def norm_back(gradient, normed_hat, inverse, gain_row):
    scaled = gradient * gain_row
    inner_sum = jnp.mean(scaled, axis=-1, keepdims=True)
    cross_sum = jnp.mean(scaled * normed_hat, axis=-1, keepdims=True)
    return inverse * (scaled - inner_sum - normed_hat * cross_sum)


def relative_onehot(window_side):
    positions = jnp.arange(window_side)
    offset_grid = positions[:, None] - positions[None, :] + (window_side - 1)
    return (offset_grid[:, :, None] == jnp.arange(2 * window_side - 1)[None, None, :]).astype(
        jnp.float32
    )


def relative(bias_table, window_side):
    onehot = relative_onehot(window_side)
    heads_count = bias_table.shape[0]
    square = bias_table.reshape(heads_count, 2 * window_side - 1, 2 * window_side - 1)
    spread_full = jnp.einsum("ija,klb,hab->hikjl", onehot, onehot, square, precision=highest)
    return spread_full.reshape(heads_count, window_side * window_side, window_side * window_side)


def relative_back(gradient, window_side):
    onehot = relative_onehot(window_side)
    heads_count = gradient.shape[0]
    grad_grid = gradient.reshape(heads_count, window_side, window_side, window_side, window_side)
    folded = jnp.einsum("hikjl,ija,klb->hab", grad_grid, onehot, onehot, precision=highest)
    return folded.reshape(heads_count, (2 * window_side - 1) ** 2)


def scatter_rows(part):
    sums = lax.psum_scatter(
        part.astype(jnp.bfloat16), "tensor", scatter_dimension=0, tiled=True
    )
    return sums.astype(jnp.float32)


def on_device(
    tokens,
    blank_mask,
    norm_gain,
    norm_bias,
    w_qkv,
    qv_bias,
    rel_bias,
    w_out,
    out_bias,
    w_up,
    up_bias,
    w_down,
    grad_out,
):
    tensor_count = lax.axis_size("tensor")
    rows_all = tokens.shape[0]
    rows_own = rows_all // tensor_count
    row_start = lax.axis_index("tensor") * rows_own
    window_area = WS * WS
    windows = rows_all // window_area
    heads_here = rel_bias.shape[0]
    width_here = w_out.shape[0]
    head_dim = width_here // heads_here
    score_scale = head_dim ** (-0.5)

    def own_rows(values):
        return lax.dynamic_slice_in_dim(values, row_start, rows_own, 0)

    source = tokens.astype(jnp.float32)
    hat_one, inv_one = normalize(source)
    normed_one = (hat_one * norm_gain[0] + norm_bias[0]).astype(jnp.bfloat16)
    projected = jnp.einsum("rd,tde->tre", normed_one, w_qkv, preferred_element_type=jnp.float32)
    shifts = jnp.stack([qv_bias[0], jnp.zeros_like(qv_bias[0]), qv_bias[1]])
    projected = (projected + shifts[:, None, :]).astype(jnp.bfloat16)
    projected = projected.reshape(3, windows, window_area, heads_here, head_dim)
    query_part, key_part, value_part = (projected[0], projected[1], projected[2])
    bias_block = relative(rel_bias, WS)

    def scores_of():
        raw_scores = jnp.einsum(
            "wihc,wjhc->whij", query_part, key_part, preferred_element_type=jnp.float32
        )
        return raw_scores * score_scale + bias_block[None]

    scores = scores_of()
    row_top = jnp.max(scores, axis=-1, keepdims=True)
    exponent = jnp.exp(scores - row_top)
    row_total = jnp.sum(exponent, axis=-1, keepdims=True)
    log_total = row_top + jnp.log(row_total)
    weights = (exponent / row_total).astype(jnp.bfloat16)
    mixed_heads = jnp.einsum(
        "whij,wjhc->wihc", weights, value_part, preferred_element_type=jnp.float32
    )
    mixed_heads = mixed_heads.astype(jnp.bfloat16).reshape(rows_all, width_here)
    attn_part = jnp.dot(mixed_heads, w_out, preferred_element_type=jnp.float32)
    alive_rows = jnp.repeat(1.0 - blank_mask.astype(jnp.float32), window_area)
    alive_own = own_rows(alive_rows)[:, None]
    source_own = own_rows(source)
    attn_own = scatter_rows(attn_part) + out_bias[0]
    resid_own = source_own + attn_own
    hat_two, inv_two = normalize(resid_own)
    normed_rows = (hat_two * norm_gain[1] + norm_bias[1]).astype(jnp.bfloat16)
    normed_two = lax.all_gather(normed_rows, "tensor", axis=0, tiled=True)
    hidden = jnp.dot(normed_two, w_up, preferred_element_type=jnp.float32) + up_bias
    active = jax.nn.gelu(hidden, approximate=False).astype(jnp.bfloat16)
    mlp_part = jnp.dot(active, w_down, preferred_element_type=jnp.float32)
    branch_own = scatter_rows(mlp_part) + out_bias[1]
    output = (resid_own + branch_own).astype(jnp.bfloat16)
    stat_terms = jnp.stack(
        [
            jnp.sum(alive_own * source_own * source_own),
            jnp.sum(alive_own * attn_own * attn_own),
            jnp.sum(alive_own * branch_own * branch_own),
            jnp.sum(alive_own),
        ]
    )
    stat_total = lax.psum(stat_terms, ("dp", "tensor"))
    grad_full = grad_out.astype(jnp.float32)
    grad_down = jnp.einsum("rf,rd->fd", active, grad_out, preferred_element_type=jnp.float32)
    grad_active = jnp.einsum("rd,fd->rf", grad_out, w_down, preferred_element_type=jnp.float32)
    gelu_slope = (
        0.5 * (1.0 + lax.erf(hidden * half_root))
        + hidden * jnp.exp(-0.5 * hidden * hidden) * gauss_norm
    )
    grad_hidden = (grad_active * gelu_slope).astype(jnp.bfloat16)
    grad_up_bias = jnp.sum(grad_hidden.astype(jnp.float32), axis=0)
    grad_up = jnp.einsum("rd,rf->df", normed_two, grad_hidden, preferred_element_type=jnp.float32)
    norm_part = jnp.einsum("rf,df->rd", grad_hidden, w_up, preferred_element_type=jnp.float32)
    grad_norm_own = scatter_rows(norm_part)
    grad_resid_own = own_rows(grad_full) + norm_back(grad_norm_own, hat_two, inv_two, norm_gain[1])
    grad_attn = lax.all_gather(grad_resid_own.astype(jnp.bfloat16), "tensor", axis=0, tiled=True)
    gain_two = jnp.sum(grad_norm_own * hat_two, axis=0)
    shift_two = jnp.sum(grad_norm_own, axis=0)
    attn_bias_term = jnp.sum(own_rows(grad_attn).astype(jnp.float32), axis=0)
    mlp_bias_term = jnp.sum(own_rows(grad_full), axis=0)
    grad_wout = jnp.einsum("re,rd->ed", mixed_heads, grad_attn, preferred_element_type=jnp.float32)
    grad_mixed = jnp.einsum("rd,ed->re", grad_attn, w_out, preferred_element_type=jnp.float32)
    grad_mixed = grad_mixed.astype(jnp.bfloat16).reshape(windows, window_area, heads_here, head_dim)
    probs_full = jnp.exp(scores_of() - log_total)
    probs_low = probs_full.astype(jnp.bfloat16)
    grad_values = jnp.einsum(
        "whij,wihc->wjhc", probs_low, grad_mixed, preferred_element_type=jnp.float32
    )
    grad_probs = jnp.einsum(
        "wihc,wjhc->whij", grad_mixed, value_part, preferred_element_type=jnp.float32
    )
    inner_sum = jnp.sum(grad_probs * probs_full, axis=-1, keepdims=True)
    grad_scores = (probs_full * (grad_probs - inner_sum)).astype(jnp.bfloat16)
    grad_table = relative_back(jnp.sum(grad_scores.astype(jnp.float32), axis=0), WS)
    grad_query = (
        jnp.einsum("whij,wjhc->wihc", grad_scores, key_part, preferred_element_type=jnp.float32)
        * score_scale
    )
    grad_keys = (
        jnp.einsum("whij,wihc->wjhc", grad_scores, query_part, preferred_element_type=jnp.float32)
        * score_scale
    )
    grad_proj = (
        jnp.stack([grad_query, grad_keys, grad_values])
        .astype(jnp.bfloat16)
        .reshape(3, rows_all, width_here)
    )
    grad_qv = jnp.stack(
        [
            jnp.sum(grad_proj[0].astype(jnp.float32), axis=0),
            jnp.sum(grad_proj[2].astype(jnp.float32), axis=0),
        ]
    )
    grad_qkv = jnp.einsum("rd,tre->tde", normed_one, grad_proj, preferred_element_type=jnp.float32)
    input_part = jnp.einsum("tre,tde->rd", grad_proj, w_qkv, preferred_element_type=jnp.float32)
    grad_in_own = scatter_rows(input_part)
    hat_one_own = own_rows(hat_one)
    grad_tokens = grad_resid_own + norm_back(
        grad_in_own, hat_one_own, own_rows(inv_one), norm_gain[0]
    )
    gain_one = jnp.sum(grad_in_own * hat_one_own, axis=0)
    shift_one = jnp.sum(grad_in_own, axis=0)
    gain_terms = jnp.stack([gain_one, gain_two])
    shift_terms = jnp.stack([shift_one, shift_two])
    bias_terms = jnp.stack([attn_bias_term, mlp_bias_term])
    gain_sums, shift_sums, bias_sums = lax.psum(
        (gain_terms, shift_terms, bias_terms), ("dp", "tensor")
    )
    grad_qv, grad_table, grad_up_bias = lax.psum((grad_qv, grad_table, grad_up_bias), "dp")
    grad_qkv, grad_wout, grad_up, grad_down = [
        total.astype(jnp.float32)
        for total in lax.psum(
            [part.astype(jnp.bfloat16) for part in (grad_qkv, grad_wout, grad_up, grad_down)],
            "dp",
        )
    ]
    live_count = jnp.maximum(stat_total[3], 1.0) * tokens.shape[1]
    root_means = jnp.sqrt(stat_total[0:3] / live_count)
    return (
        output,
        grad_tokens,
        gain_sums,
        shift_sums,
        grad_qkv,
        grad_qv,
        grad_table,
        grad_wout,
        bias_sums,
        grad_up,
        grad_up_bias,
        grad_down,
        root_means,
    )


def on_block(
    tokens,
    blank_mask,
    norm_gain,
    norm_bias,
    w_qkv,
    qv_bias,
    rel_bias,
    w_out,
    out_bias,
    w_up,
    up_bias,
    w_down,
    grad_out,
):
    count = lax.axis_size("tensor")
    depth = tokens.shape[1]
    area = WS * WS
    rows = -(-area // ROW_TILE) * ROW_TILE
    windows = tokens.shape[0] // area
    subs = windows // count
    own = subs * rows
    here = lax.axis_index("tensor")
    heads_here = rel_bias.shape[0]
    width_here = w_out.shape[0]
    head_dim = width_here // heads_here
    score_scale = head_dim ** (-0.5)
    half = jnp.bfloat16
    rows_all = windows * rows

    def padded(values):
        return jnp.pad(
            values.reshape(windows, area, depth), ((0, 0), (0, rows - area), (0, 0))
        ).reshape(count, own, depth)

    def own_rows(values):
        return lax.dynamic_index_in_dim(values, here, 0, keepdims=False)

    def stripped(values):
        return values.reshape(subs, rows, depth)[:, :area].reshape(subs * area, depth)

    source_low = padded(tokens)
    cot = padded(grad_out)
    source = source_low.reshape(rows_all, depth).astype(jnp.float32)
    hat_one, inv_one = normalize(source)
    normed_one = (hat_one * norm_gain[0] + norm_bias[0]).astype(half)
    projected = jnp.einsum("rd,tde->tre", normed_one, w_qkv, preferred_element_type=jnp.float32)
    shifts = jnp.stack([qv_bias[0], jnp.zeros_like(qv_bias[0]), qv_bias[1]])
    projected = (projected + shifts[:, None, :]).astype(half)
    projected = projected.reshape(3, windows, rows, heads_here, head_dim)
    query_part, key_part, value_part = (projected[0], projected[1], projected[2])
    bias_block = jnp.pad(
        jnp.pad(
            relative(rel_bias, WS), ((0, 0), (0, 0), (0, rows - area)), constant_values=-1e30
        ),
        ((0, 0), (0, rows - area), (0, 0)),
    )

    def scores_of():
        raw_scores = jnp.einsum(
            "wihc,wjhc->whij", query_part, key_part, preferred_element_type=jnp.float32
        )
        return raw_scores * score_scale + bias_block[None]

    scores = scores_of()
    row_top = jnp.max(scores, axis=-1, keepdims=True)
    exponent = jnp.exp(scores - row_top)
    row_total = jnp.sum(exponent, axis=-1, keepdims=True)
    log_total = row_top + jnp.log(row_total)
    weights = (exponent / row_total).astype(half)
    mixed_heads = jnp.einsum(
        "whij,wjhc->wihc", weights, value_part, preferred_element_type=jnp.float32
    )
    mixed_heads = mixed_heads.astype(half).reshape(rows_all, width_here)
    attn_part = (
        jnp.dot(mixed_heads, w_out, preferred_element_type=jnp.float32)
        .astype(half)
        .reshape(count, own, depth)
    )
    alive = own_rows((1.0 - blank_mask.astype(jnp.float32)).reshape(count, subs))
    inside = (jnp.arange(rows) < area).astype(jnp.float32)
    live = (alive[:, None] * inside[None, :]).reshape(own, 1)
    output, grad_resid_own, grad_attn, low_grads, sums = middle(
        count,
        attn_part,
        own_rows(source_low),
        live,
        norm_gain,
        norm_bias,
        out_bias,
        w_up,
        up_bias[None],
        w_down,
        cot,
        subs,
        rows,
    )
    grad_down = low_grads[0].reshape(w_down.shape).astype(jnp.float32)
    grad_up = low_grads[1].reshape(w_up.shape).astype(jnp.float32)
    grad_attn = grad_attn.reshape(rows_all, depth)
    grad_wout = jnp.einsum("re,rd->ed", mixed_heads, grad_attn, preferred_element_type=jnp.float32)
    grad_mixed = jnp.einsum("rd,ed->re", grad_attn, w_out, preferred_element_type=jnp.float32)
    grad_mixed = grad_mixed.astype(half).reshape(windows, rows, heads_here, head_dim)
    probs_full = jnp.exp(scores_of() - log_total)
    probs_low = probs_full.astype(half)
    grad_values = jnp.einsum(
        "whij,wihc->wjhc", probs_low, grad_mixed, preferred_element_type=jnp.float32
    )
    grad_probs = jnp.einsum(
        "wihc,wjhc->whij", grad_mixed, value_part, preferred_element_type=jnp.float32
    )
    inner_sum = jnp.sum(grad_probs * probs_full, axis=-1, keepdims=True)
    grad_scores = (probs_full * (grad_probs - inner_sum)).astype(half)
    grad_table = relative_back(
        jnp.sum(grad_scores.astype(jnp.float32), axis=0)[:, :area, :area], WS
    )
    grad_query = (
        jnp.einsum("whij,wjhc->wihc", grad_scores, key_part, preferred_element_type=jnp.float32)
        * score_scale
    )
    grad_keys = (
        jnp.einsum("whij,wihc->wjhc", grad_scores, query_part, preferred_element_type=jnp.float32)
        * score_scale
    )
    grad_proj = (
        jnp.stack([grad_query, grad_keys, grad_values])
        .astype(half)
        .reshape(3, rows_all, width_here)
    )
    grad_qv = jnp.stack(
        [
            jnp.sum(grad_proj[0].astype(jnp.float32), axis=0),
            jnp.sum(grad_proj[2].astype(jnp.float32), axis=0),
        ]
    )
    grad_qkv = jnp.einsum("rd,tre->tde", normed_one, grad_proj, preferred_element_type=jnp.float32)
    input_part = jnp.einsum("tre,tde->rd", grad_proj, w_qkv, preferred_element_type=jnp.float32)
    grad_in_own = scatter_rows(input_part)
    hat_one_own = own_rows(hat_one.reshape(count, own, depth))
    inv_one_own = own_rows(inv_one.reshape(count, own, 1))
    grad_tokens = grad_resid_own + norm_back(grad_in_own, hat_one_own, inv_one_own, norm_gain[0])
    gain_one = jnp.sum(input_part * hat_one, axis=0)
    shift_one = jnp.sum(input_part, axis=0)
    gain_terms = jnp.stack([gain_one, sums[0]])
    shift_terms = jnp.stack([shift_one, sums[1]])
    stat_terms = jnp.concatenate([jnp.sum(sums[5:8], axis=1), jnp.sum(alive)[None] * area])
    gain_sums, shift_sums, bias_sums, stat_total = lax.psum(
        (gain_terms, shift_terms, sums[2:4], stat_terms), ("dp", "tensor")
    )
    grad_qv, grad_table, grad_up_bias = lax.psum((grad_qv, grad_table, sums[4]), "dp")
    grad_qkv, grad_wout = [
        total.astype(jnp.float32)
        for total in lax.psum([part.astype(half) for part in (grad_qkv, grad_wout)], "dp")
    ]
    live_count = jnp.maximum(stat_total[3], 1.0) * depth
    root_means = jnp.sqrt(stat_total[0:3] / live_count)
    return (
        stripped(output),
        stripped(grad_tokens),
        gain_sums,
        shift_sums,
        grad_qkv,
        grad_qv,
        grad_table,
        grad_wout,
        bias_sums,
        grad_up,
        grad_up_bias,
        grad_down,
        root_means,
    )


def solution(mesh):
    in_specs = (
        P("dp", None),
        P("dp"),
        P(),
        P(),
        P(None, None, "tensor"),
        P(None, "tensor"),
        P("tensor", None),
        P("tensor", None),
        P(),
        P(None, "tensor"),
        P("tensor"),
        P("tensor", None),
        P("dp", None),
    )
    out_specs = (
        P(("dp", "tensor"), None),
        P(("dp", "tensor"), None),
        P(),
        P(),
        P(None, None, "tensor"),
        P(None, "tensor"),
        P("tensor", None),
        P("tensor", None),
        P(),
        P(None, "tensor"),
        P("tensor"),
        P("tensor", None),
        P(),
    )
    fits = mesh.shape["tensor"] == 4 and mesh.shape["dp"] == 8
    return jax.shard_map(
        on_block if fits else on_device, mesh=mesh, in_specs=in_specs, out_specs=out_specs, check_vma=False
    )
```
